32 devices in a mesh: site: 16 (over z, x, core), sec: 2 (over y).
Axes of the slice: x: 2, y: 2, z: 4, core: 2. Of those that a mesh axis runs over, the one named last changes fastest.
Arguments:
- left_canon: bfloat16 [16, 4, 4, 128, 128], P('site', None, 'sec'), may hold values from -1.5 to 1.5
- right_canon: bfloat16 [16, 4, 4, 128, 128], P('site', None, 'sec'), may hold values from -1.5 to 1.5
- center_site: bfloat16 [16, 4, 4, 128, 128], P('site', None, 'sec'), may hold values from -6 to 6
- center_bond: bfloat16 [16, 4, 128, 128], P('site', 'sec'), may hold values from -2 to 3
- left_seed: bfloat16 [16, 4, 128, 128], P('site', 'sec'), may hold values from -2 to 4
- right_seed: bfloat16 [16, 4, 128, 128], P('site', 'sec'), may hold values from -2 to 4
- left_sector: int32 [16, 4, 4], P('site'), may hold values from 0 to 3, each once within a row
- onsite: float32 [16, 4], P('site'), may hold values from 0.5 to 2
- bond_shift: float32 [16], P('site'), may hold values from 0.5 to 2
Outputs:
- left_new: bfloat16 [16, 4, 4, 128, 128], P('site', None, 'sec')
- right_new: bfloat16 [16, 4, 4, 128, 128], P('site', None, 'sec')
The draws below stay inside these ranges and needn't reach their ends.
Inputs may be any that keep to these rules, and one draw needn't show every extreme that they name: `left_sector`: for each site and local state the 4 entries are a permutation of the sectors.
All inputs are finite; a program needn't handle non-finite values.
Results may differ from the reference program's by a relative error of at most 0.028.
Values may be sent and summed in bfloat16 or wider, within the bound.
No kernel may reach another device: no remote copies, remote signals or barrier semaphores. Data moves between devices by JAX's collectives and lax.ppermute only.
A program may use at most 64 MiB of HBM per device.

```python
import math
import jax
import jax.numpy as jnp
from jax import lax

B = 128
PHYS = 4
NSI = 10
NAPP = 2
SITES = 16
NSEC = 4
RCH = 4


def noise_shaped(key, shape):
    values = jnp.clip(jax.random.normal(key, shape, jnp.float32), -4.0, 4.0)
    return values


def noise_field(key):
    return noise_shaped(key, (SITES, NSEC, B, B))


def canon_tensor(key):
    values = noise_shaped(jax.random.fold_in(key, 3), (SITES, PHYS, NSEC, B, B))
    leading = jax.random.randint(jax.random.fold_in(key, 5), (SITES,), 0, PHYS)
    states = jnp.arange(PHYS, dtype=jnp.int32)
    weights = jnp.where(states[None, :] == leading[:, None], 0.9, 0.2).astype(jnp.float32)
    identity = jnp.eye(B, dtype=jnp.float32)
    return (weights[:, :, None, None, None] * identity + 0.25 / math.sqrt(B) * values).astype(jnp.bfloat16)


def symmetric_seed(key):
    values = noise_field(jax.random.fold_in(key, 1))
    mixed = (values + jnp.swapaxes(values, -1, -2)) * 0.70710678
    levels = jnp.exp(jax.random.uniform(jax.random.fold_in(key, 2), (SITES, NSEC), jnp.float32, math.log(0.5), math.log(2.0)))
    blocks = jnp.eye(B, dtype=jnp.float32) + 0.5 / math.sqrt(B) * mixed
    return (levels[:, :, None, None] * blocks).astype(jnp.bfloat16)


def draw_left_canon(key, part):
    return canon_tensor(jax.random.fold_in(key, 41))


def draw_right_canon(key, part):
    return canon_tensor(jax.random.fold_in(key, 53))


def draw_center_bond(key, part):
    values = noise_field(jax.random.fold_in(key, 11))
    return (jnp.eye(B, dtype=jnp.float32) + 0.3 / math.sqrt(B) * values).astype(jnp.bfloat16)


def draw_left_seed(key, part):
    return symmetric_seed(jax.random.fold_in(key, 23))


def draw_right_seed(key, part):
    return symmetric_seed(jax.random.fold_in(key, 37))


def shard_levels(key, dims, shards, smallest, largest):
    gain, own = 1.0, jax.random.fold_in(key, 6)
    for position, shards_of in shards:
        draws = jnp.exp(jax.random.uniform(jax.random.fold_in(own, position), (shards_of,), jnp.float32, smallest / len(shards), largest / len(shards)))
        gain = gain * jnp.repeat(draws, dims[position] // shards_of).reshape([-1 if axis == position else 1 for axis in range(len(dims))])
    return gain


def bell_draw(own_key, shape, width, bound, pieces=(), kind=jnp.bfloat16):
    drawn = jax.random.normal(own_key, shape, jnp.float32) * width
    if len(pieces) > 0:
        drawn = shard_levels(own_key, shape, pieces, -0.22, 0.18) * drawn
    return jnp.clip(drawn, min=-bound, max=bound).astype(kind)


def setup_inputs(seed: int = 0) -> dict:
    keys = jax.random.split(jax.random.key(seed), 10)
    left_canon = draw_left_canon(jax.random.fold_in(keys[9], 71), 0)
    right_canon = draw_right_canon(jax.random.fold_in(keys[9], 71), 0)
    center_site = bell_draw(keys[2], (SITES, PHYS, NSEC, B, B), 1.0, 6.0, ((0, 16), (2, 2)))
    center_bond = draw_center_bond(jax.random.fold_in(keys[9], 71), 0)
    left_seed = draw_left_seed(jax.random.fold_in(keys[9], 71), 0)
    right_seed = draw_right_seed(jax.random.fold_in(keys[9], 71), 0)
    left_sector = jax.vmap(lambda own: jax.random.permutation(own, NSEC))(jax.random.split(keys[6], SITES * PHYS)).reshape((SITES, PHYS, NSEC)).astype(jnp.int32)
    onsite = jnp.clip(jnp.exp(math.log(2.0) - 1.3862944 * jax.random.uniform(keys[7], (SITES, PHYS), jnp.float32) ** shard_levels(keys[7], (SITES, PHYS), ((0, 16),), -0.2, 0.2)), 0.5, 2.0)
    bond_shift = jnp.clip(jnp.exp(math.log(2.0) - 1.3862944 * jax.random.uniform(keys[8], (SITES,), jnp.float32) ** shard_levels(keys[8], (SITES,), ((0, 16),), -0.2, 0.2)), 0.5, 2.0)
    return {"left_canon": left_canon, "right_canon": right_canon, "center_site": center_site, "center_bond": center_bond, "left_seed": left_seed, "right_seed": right_seed, "left_sector": left_sector, "onsite": onsite, "bond_shift": bond_shift}


def pick_blocks(blocks, indices):
    return jax.vmap(lambda chosen, where_at: jnp.take(chosen, where_at, axis=0))(blocks, indices)

def inverse_root(gram_mat):
    scaling = jnp.sqrt(lax.optimization_barrier(jnp.sum(gram_mat * gram_mat, axis=(-2, -1), keepdims=True)))
    identity = jnp.eye(gram_mat.shape[-1], dtype=jnp.float32)
    upper_part = gram_mat / scaling
    lower_part = jnp.broadcast_to(identity, gram_mat.shape)
    for repeat in range(NSI):
        middle = 1.5 * identity - 0.5 * jnp.matmul(lower_part, upper_part, precision=lax.Precision.HIGHEST)
        upper_part = jnp.matmul(upper_part, middle, precision=lax.Precision.HIGHEST)
        lower_part = jnp.matmul(middle, lower_part, precision=lax.Precision.HIGHEST)
    return lower_part / jnp.sqrt(scaling)

def trace_sum(blocks):
    return lax.optimization_barrier(jnp.sum(jnp.diagonal(blocks.astype(jnp.float32), axis1=2, axis2=3), axis=(1, 2)))

def reference(left_canon, right_canon, center_site, center_bond, left_seed, right_seed, left_sector, onsite, bond_shift):
    labels = jnp.arange(NSEC, dtype=jnp.int32)
    right_of = lax.optimization_barrier(jnp.sum(jnp.where(left_sector[:, :, :, None] == labels[None, None, None, :], labels[None, None, :, None], 0), axis=2)).astype(jnp.int32)
    routing = (left_sector[:, :, :, None] == labels[None, None, None, :]).astype(jnp.float32)

    def left_step(hold):
        running = jnp.zeros(hold.shape, jnp.float32)
        for physical in range(PHYS):
            tensor = left_canon[:, physical].astype(jnp.float32)
            chosen = pick_blocks(hold, left_sector[:, physical]).astype(jnp.float32)
            product = jnp.einsum('jkab,jkbc->jkac', chosen, tensor).astype(jnp.bfloat16)
            running = running + jnp.einsum('jkba,jkbc->jkac', tensor, product.astype(jnp.float32))
        return running.astype(jnp.bfloat16)

    def right_step(hold):
        running = jnp.zeros(hold.shape, jnp.float32)
        for physical in range(PHYS):
            picked = pick_blocks(right_canon[:, physical], right_of[:, physical]).astype(jnp.float32)
            env_chosen = pick_blocks(hold, right_of[:, physical]).astype(jnp.float32)
            product = jnp.einsum('jkab,jkbc->jkac', picked, env_chosen).astype(jnp.bfloat16)
            running = running + jnp.einsum('jkac,jkdc->jkad', product.astype(jnp.float32), picked)
        return running.astype(jnp.bfloat16)
    left_hold = left_seed
    right_hold = right_seed
    left_fresh = left_seed
    for step in range(RCH):
        left_fresh = left_step(left_hold)
        right_fresh = right_step(right_hold)
        left_hold = jnp.roll(left_fresh, 1, axis=0)
        right_hold = jnp.roll(right_fresh, -1, axis=0)
    dim_all = NSEC * B

    def scaled(blocks):
        return (blocks.astype(jnp.float32) * (dim_all / trace_sum(blocks))[:, None, None, None]).astype(jnp.bfloat16)
    cur_scaled = scaled(left_hold)
    next_scaled = scaled(left_fresh)
    right_scaled = scaled(right_hold)
    chosen_left = pick_blocks(cur_scaled, left_sector).astype(jnp.float32)
    site_now = center_site
    bond_now = center_bond
    for repeat in range(NAPP):
        half_site = jnp.einsum('jskab,jskbc->jskac', chosen_left, site_now.astype(jnp.float32)).astype(jnp.bfloat16)
        site_now = (jnp.einsum('jskab,jkbc->jskac', half_site.astype(jnp.float32), right_scaled.astype(jnp.float32)) + onsite[:, :, None, None, None] * site_now.astype(jnp.float32)).astype(jnp.bfloat16)
        half_bond = jnp.einsum('jkab,jkbc->jkac', next_scaled.astype(jnp.float32), bond_now.astype(jnp.float32)).astype(jnp.bfloat16)
        bond_now = (jnp.einsum('jkab,jkbc->jkac', half_bond.astype(jnp.float32), right_scaled.astype(jnp.float32)) + bond_shift[:, None, None, None] * bond_now.astype(jnp.float32)).astype(jnp.bfloat16)
    site_wide = site_now.astype(jnp.float32)
    bond_wide = bond_now.astype(jnp.float32)
    gram_left = jnp.einsum('jskab,jskac->jkbc', site_wide, site_wide)
    gram_bond = jnp.einsum('jkab,jkac->jkbc', bond_wide, bond_wide)
    unit_left = jnp.matmul(bond_wide, inverse_root(gram_bond), precision=lax.Precision.HIGHEST)
    factor_left = jnp.matmul(inverse_root(gram_left), jnp.swapaxes(unit_left, -1, -2), precision=lax.Precision.HIGHEST).astype(jnp.bfloat16)
    left_new = jnp.einsum('jskab,jkbc->jskac', site_wide, factor_left.astype(jnp.float32)).astype(jnp.bfloat16)
    outer_terms = jnp.einsum('jskab,jskcb->jskac', site_wide, site_wide)
    gram_right = jnp.einsum('jskm,jskac->jmac', routing, outer_terms)
    previous = jnp.roll(bond_now, 1, axis=0).astype(jnp.float32)
    gram_prev = jnp.matmul(previous, jnp.swapaxes(previous, -1, -2), precision=lax.Precision.HIGHEST)
    unit_right = jnp.matmul(inverse_root(gram_prev), previous, precision=lax.Precision.HIGHEST)
    factor_right = jnp.matmul(jnp.swapaxes(unit_right, -1, -2), inverse_root(gram_right), precision=lax.Precision.HIGHEST).astype(jnp.bfloat16)
    factor_chosen = pick_blocks(factor_right, left_sector).astype(jnp.float32)
    right_new = jnp.einsum('jskab,jskbc->jskac', factor_chosen, site_wide).astype(jnp.bfloat16)
    return (left_new, right_new)
```

```python
import functools

import jax
import jax.numpy as jnp
from jax import lax
from jax.experimental import pallas as pl
from jax.experimental.pallas import tpu as pltpu
from jax.sharding import PartitionSpec as P

NSI = 10
NAPP = 2
f32 = jnp.float32
bf16 = jnp.bfloat16
VMEM = pl.BlockSpec(memory_space=pltpu.VMEM)
SMEM = pl.BlockSpec(memory_space=pltpu.SMEM)
ANY = pl.BlockSpec(memory_space=pl.ANY)


def dot(a, b):
    return jnp.dot(a, b, preferred_element_type=f32)


def dot_tn(a, b):
    return lax.dot_general(a, b, (((0,), (0,)), ((), ())), preferred_element_type=f32)


def dot_nt(a, b):
    return lax.dot_general(a, b, (((1,), (1,)), ((), ())), preferred_element_type=f32)


def split(x):
    high = x.astype(bf16)
    low = (x - high.astype(f32)).astype(bf16)
    return jnp.concatenate([high, low], axis=1)


def twice(s):
    return jnp.concatenate([s, s], axis=0)


def fold(x):
    width = x.shape[1] // 2
    return x[:, :width] + x[:, width:]


def eye(width):
    rows = lax.broadcasted_iota(jnp.int32, (width, width), 0)
    cols = lax.broadcasted_iota(jnp.int32, (width, width), 1)
    return (rows == cols).astype(f32)


def total(x):
    return jnp.sum(jnp.sum(x, axis=0, keepdims=True), axis=1, keepdims=True)


class Table:
    def __init__(self, ref, phys, n):
        self.ref, self.phys, self.n = ref, phys, n

    def src(self, g, s, k):
        return self.ref[((g * 2) * self.phys + s) * self.n + k]

    def dst(self, g, s, m):
        return self.ref[((g * 2 + 1) * self.phys + s) * self.n + m]


def gather_states(blocks, table, g, m, phys):
    return jnp.concatenate([blocks[s, table.dst(g, s, m)] for s in range(phys)], axis=1)


def scatter_states(store, product, table, g, m, phys, width):
    for s in range(phys):
        store[table.dst(g, s, m), s * width : (s + 1) * width, :] = product[
            :, s * width : (s + 1) * width
        ]


def chain_kernel(dims, first, last, tab_ref, pos_ref, *refs):
    hops, sizes, phys, n, own, width = dims
    count = hops * sizes
    local_left, local_right = refs[0], refs[1]
    moved = (None,) + refs[2 : 2 + count - 1]
    rest = refs[2 + count - 1 :]
    if not first:
        env_in, rest = rest[0], rest[1:]
    elif hops == 1:
        seeds, rest = rest[:2], rest[2:]
    out_ref, blocks, env, wide, tall, sems = rest
    table = Table(tab_ref, phys, n)
    pos = pos_ref[0]

    def slot(t):
        return pl.ds(lax.rem(pos - t + sizes, sizes) * own, own)

    def copies(local):
        found = []
        for g in range(hops):
            for t in range(sizes):
                i = g * sizes + t
                source = local if i == 0 else moved[i].at[pl.ds(0, phys)]
                found.append(
                    pltpu.make_async_copy(source, blocks.at[g, :, slot(t)], sems.at[i])
                )
        return found

    def seed_copies(local):
        found = []
        for t in range(sizes):
            i = (hops - 1) * sizes + t
            source = local if i == 0 else moved[i].at[phys]
            found.append(pltpu.make_async_copy(source, env.at[slot(t)], sems.at[count + t]))
        return found

    def run(local, seed, step):
        loads = copies(local)
        starts = seed_copies(seed) if first else []
        for copy in starts + loads:
            copy.start()
        if not first:
            env[...] = env_in[...]
        for copy in starts:
            copy.wait()
        for g in reversed(range(hops)):
            for copy in loads[g * sizes : (g + 1) * sizes]:
                copy.wait()
            step(g)

    def left_step(g):
        for m in range(n):
            product = dot(env[m], gather_states(blocks.at[g], table, g, m, phys)).astype(bf16)
            scatter_states(tall, product, table, g, m, phys, width)
        for k in range(n):
            stacked = blocks[g, :, k].reshape(phys * width, width)
            env[k] = dot_tn(stacked, tall[k]).astype(bf16)

    def right_step(g):
        for k in range(n):
            stacked = blocks[g, :, k].reshape(phys * width, width)
            product = dot(stacked, env[k]).astype(bf16)
            for s in range(phys):
                wide[table.src(g, s, k), :, s * width : (s + 1) * width] = product[
                    s * width : (s + 1) * width
                ]
        for m in range(n):
            env[m] = dot_nt(wide[m], gather_states(blocks.at[g], table, g, m, phys)).astype(bf16)

    local_seeds = seeds if first and hops == 1 else (None, None)

    @pl.when(pos < sizes // 2)
    def _():
        run(local_left, local_seeds[0], left_step)

    @pl.when(pos >= sizes // 2)
    def _():
        run(local_right, local_seeds[1], right_step)

    if last:
        summed = env[0].astype(f32)
        for m in range(1, n):
            summed = summed + env[m].astype(f32)
        scale = (n * width) / total(summed * eye(width))
        for m in range(n):
            out_ref[m] = (env[m].astype(f32) * scale).astype(bf16)
    else:
        out_ref[...] = env[...]


def center_kernel(dims, tab_ref, pos_ref, onsite_ref, shift_ref, *refs):
    sizes, phys, n, own, width = dims
    same_ref, cross_ref, mine_ref, swap_ref, bond_ref = refs[:5]
    site_parts = refs[5 : 5 + sizes]
    bond_parts = refs[5 + sizes : 5 + 2 * sizes]
    left_out, right_out = refs[5 + 2 * sizes : 7 + 2 * sizes]
    site, envs, bonds, tall, y_ref, z_ref, m_ref, scale_ref, factor_ref, sems = refs[
        7 + 2 * sizes :
    ]
    table = Table(tab_ref, phys, n)
    pos = pos_ref[0]
    on_right = (pos >= sizes // 2).astype(jnp.int32)

    def slot(t, extra=0):
        return pl.ds(extra + lax.rem(pos - t + sizes, sizes) * own, own)

    copies = []
    for t in range(sizes):
        copies.append(
            pltpu.make_async_copy(site_parts[t], site.at[:, slot(t)], sems.at[t])
        )
        copies.append(
            pltpu.make_async_copy(bond_parts[t], bonds.at[slot(t, own)], sems.at[sizes + t])
        )
    targets = (
        (same_ref, on_right),
        (cross_ref, 1 - on_right),
        (mine_ref, 3 - on_right),
        (swap_ref, 2 + on_right),
    )
    for i, (ref, where) in enumerate(targets):
        copies.append(pltpu.make_async_copy(ref, envs.at[where], sems.at[2 * sizes + i]))
    for copy in copies:
        copy.start()
    bonds[0:own] = bond_ref[...]
    for copy in copies:
        copy.wait()

    for repeat in range(NAPP):
        for m in range(n):
            product = dot(envs[0, m], gather_states(site, table, 0, m, phys)).astype(bf16)
            scatter_states(tall, product, table, 0, m, phys, width)
        for i in range(own):
            k = pos * own + i
            half = dot(envs[3, k], bonds[i]).astype(bf16)
            bonds[i] = (dot(half, envs[1, k]) + shift_ref[0] * bonds[i].astype(f32)).astype(bf16)
        for m in range(n):
            half = dot(envs[0, m], bonds[own + m]).astype(bf16)
            bonds[own + m] = (
                dot(half, envs[2, m]) + shift_ref[1] * bonds[own + m].astype(f32)
            ).astype(bf16)
        for k in range(n):
            product = dot(tall[k], envs[1, k])
            for s in range(phys):
                site[s, k] = (
                    product[s * width : (s + 1) * width] + onsite_ref[s] * site[s, k].astype(f32)
                ).astype(bf16)

    count = 2 * (own + n)

    def gram(i):
        if i < own + n:
            return dot_nt(bonds[i], bonds[i])
        i -= own + n
        if i < own:
            stacked = site[:, pos * own + i].reshape(phys * width, width)
            return dot_tn(stacked, stacked)
        gathered = gather_states(site, table, 0, i - own, phys)
        return dot_nt(gathered, gathered)

    for i in range(count):
        g = gram(i)
        inverse = lax.rsqrt(total(g * g))
        scale_ref[i] = jnp.broadcast_to(jnp.sqrt(inverse), scale_ref.shape[1:])
        y = g * inverse
        y_ref[i] = split(y)
        z_ref[i] = split(1.5 * eye(width) - 0.5 * y)
    for i in range(count):
        y_ref[i] = split(fold(dot(z_ref[i], twice(y_ref[i]))))

    def middle():
        for i in range(count):
            m_ref[i] = split(1.5 * eye(width) - 0.5 * fold(dot(z_ref[i], twice(y_ref[i]))))

    def finish():
        for i in range(count):
            z_ref[i] = split(fold(dot(m_ref[i], twice(z_ref[i]))))

    def iterate(step, carry):
        middle()
        for i in range(count):
            y_ref[i] = split(fold(dot(m_ref[i], twice(y_ref[i]))))
        finish()
        return carry

    lax.fori_loop(0, NSI - 2, iterate, 0)
    middle()
    finish()

    for i in range(own + n):
        unit = dot(z_ref[i], twice(bonds[i])) * scale_ref[i][:1]
        y_ref[i] = split(unit)
    for i in range(own + n):
        grams = own + n + i
        parts = y_ref[i]
        if i < own:
            high, low = parts[:, :width], parts[:, width:]
            rows = jnp.concatenate(
                [
                    jnp.concatenate([high, high], axis=1),
                    jnp.concatenate([low, low], axis=1),
                ],
                axis=0,
            )
            factor = fold(dot_nt(z_ref[grams], rows)) * scale_ref[grams][:1]
        else:
            factor = jnp.transpose(fold(dot(z_ref[grams], twice(parts))) * scale_ref[grams][:1])
        factor_ref[i] = factor.astype(bf16)
    for i in range(own):
        k = pos * own + i
        stacked = site[:, k].reshape(phys * width, width)
        product = dot(stacked, factor_ref[i]).astype(bf16)
        for s in range(phys):
            left_out[s, i] = product[s * width : (s + 1) * width]
            right_out[s, i] = dot(factor_ref[own + table.src(0, s, k)], site[s, k]).astype(bf16)


def route(mesh_shape, target):
    sites, sizes = mesh_shape
    pairs = []
    for j in range(sites):
        for c in range(sizes):
            to = target(j, c)
            if to is not None:
                pairs.append((j * sizes + c, (to[0] % sites) * sizes + to[1] % sizes))
    return pairs


def per_device(
    mesh_shape,
    left_canon,
    right_canon,
    center_site,
    center_bond,
    left_seed,
    right_seed,
    left_sector,
    onsite,
    bond_shift,
):
    sites, sizes = mesh_shape
    half = sizes // 2
    steps = sites // 4
    hops = 2 if steps % 2 == 0 else 1
    left, right = left_canon[0], right_canon[0]
    phys, own, width = left.shape[0], left.shape[1], left.shape[2]
    src = left_sector[0]
    n = src.shape[1]
    labels = jnp.arange(n, dtype=jnp.int32)
    dst = jnp.sum(
        jnp.where(src[:, :, None] == labels[None, None, :], labels[None, :, None], 0), axis=1
    )
    tab = jnp.stack([src, dst]).reshape(-1)
    pos = lax.axis_index("sec").astype(jnp.int32)
    params = pltpu.CompilerParams(vmem_limit_bytes=56 * 2**20)

    def move(x, target):
        return lax.ppermute(x, ("site", "sec"), route(mesh_shape, target))

    def outward(c, g):
        return g if c < half else -g

    moved, tables = [], [tab]
    for g in range(hops):
        for t in range(sizes):
            if g == 0 and t == 0:
                continue
            to_left = lax.rem(pos + t, sizes) < half
            payload = jnp.where(to_left, left, right)
            if g == hops - 1:
                seed = jnp.where(to_left, left_seed[0], right_seed[0])
                payload = jnp.concatenate([payload, seed[None]], axis=0)
            moved.append(
                move(payload, lambda j, c, g=g, t=t: (j + outward((c + t) % sizes, g), c + t))
            )
        if g > 0:
            tables.append(move(tab, lambda j, c, g=g: (j + outward(c, g), c)))
    tables = jnp.concatenate(tables)
    shift_before = move(bond_shift, lambda j, c: (j + 1, c))

    dims = (hops, sizes, phys, n, own, width)
    env_shape = jax.ShapeDtypeStruct((n, width, width), bf16)
    count = hops * sizes
    env = None
    blocks_total = steps // hops
    for b in range(blocks_total):
        first, last = b == 0, b == blocks_total - 1
        extra, specs = (), []
        if not first:
            extra, specs = (env,), [VMEM]
        elif hops == 1:
            extra, specs = (left_seed[0], right_seed[0]), [ANY, ANY]
        env = pl.pallas_call(
            functools.partial(chain_kernel, dims, first, last),
            out_shape=env_shape,
            in_specs=[SMEM, SMEM] + [ANY] * (count + 1) + specs,
            out_specs=VMEM,
            scratch_shapes=[
                pltpu.VMEM((hops, phys, n, width, width), bf16),
                pltpu.VMEM((n, width, width), bf16),
                pltpu.VMEM((n, width, phys * width), bf16),
                pltpu.VMEM((n, phys * width, width), bf16),
                pltpu.SemaphoreType.DMA((count + sizes,)),
            ],
            compiler_params=params,
            name="chain_last" if last else "chain",
        )(tables, pos[None], left, right, *moved, *extra)
        if first:
            center, bond, _ = lax.optimization_barrier((center_site[0], center_bond[0], env))
            center_parts = [center_site[0]] + [
                move(center, lambda j, c, t=t: (j, c + t)) for t in range(1, sizes)
            ]
            bond_parts = [move(bond, lambda j, c, t=t: (j + 1, c + t)) for t in range(sizes)]
        if not last:
            env = move(env, lambda j, c: (j + outward(c, hops), c))

    same = move(env, lambda j, c: (j + outward(c, 1), c))
    cross = move(env, lambda j, c: (j + outward(c, 1), c + half))
    swap = move(env, lambda j, c: (j, c + half))

    matrices = 2 * (own + n)
    out_shape = jax.ShapeDtypeStruct((phys, own, width, width), bf16)
    left_new, right_new = pl.pallas_call(
        functools.partial(center_kernel, (sizes, phys, n, own, width)),
        out_shape=(out_shape, out_shape),
        in_specs=[SMEM] * 4 + [ANY] * 4 + [VMEM] + [ANY] * (2 * sizes),
        out_specs=(VMEM, VMEM),
        scratch_shapes=[
            pltpu.VMEM((phys, n, width, width), bf16),
            pltpu.VMEM((4, n, width, width), bf16),
            pltpu.VMEM((own + n, width, width), bf16),
            pltpu.VMEM((n, phys * width, width), bf16),
            pltpu.VMEM((matrices, width, 2 * width), bf16),
            pltpu.VMEM((matrices, width, 2 * width), bf16),
            pltpu.VMEM((matrices, width, 2 * width), bf16),
            pltpu.VMEM((matrices, 8, width), f32),
            pltpu.VMEM((own + n, width, width), bf16),
            pltpu.SemaphoreType.DMA((2 * sizes + 4,)),
        ],
        compiler_params=params,
        name="center",
    )(
        tab,
        pos[None],
        onsite[0],
        jnp.concatenate([bond_shift, shift_before]),
        same,
        cross,
        env,
        swap,
        center_bond[0],
        *center_parts,
        *bond_parts,
    )
    return (left_new[None], right_new[None])


def solution(mesh):
    mesh_shape = (mesh.shape["site"], mesh.shape["sec"])
    return jax.shard_map(
        functools.partial(per_device, mesh_shape),
        mesh=mesh,
        in_specs=(
            P("site", None, "sec", None, None),
            P("site", None, "sec", None, None),
            P("site", None, "sec", None, None),
            P("site", "sec", None, None),
            P("site", "sec", None, None),
            P("site", "sec", None, None),
            P("site", None, None),
            P("site", None),
            P("site"),
        ),
        out_specs=(P("site", None, "sec", None, None), P("site", None, "sec", None, None)),
        check_vma=False,
    )
```

```python
import functools

import jax
import jax.numpy as jnp
from jax import lax
from jax.experimental import pallas as pl
from jax.experimental.pallas import tpu as pltpu
from jax.sharding import PartitionSpec as P

NSI = 10
NAPP = 2
f32 = jnp.float32
bf16 = jnp.bfloat16
VMEM = pl.BlockSpec(memory_space=pltpu.VMEM)
SMEM = pl.BlockSpec(memory_space=pltpu.SMEM)


def dot(a, b):
    return jnp.dot(a, b, preferred_element_type=f32)


def dot_tn(a, b):
    return lax.dot_general(a, b, (((0,), (0,)), ((), ())), preferred_element_type=f32)


def dot_nt(a, b):
    return lax.dot_general(a, b, (((1,), (1,)), ((), ())), preferred_element_type=f32)


def split(x):
    high = x.astype(bf16)
    low = (x - high.astype(f32)).astype(bf16)
    return jnp.concatenate([high, low], axis=1)


def twice(s):
    return jnp.concatenate([s, s], axis=0)


def fold(x):
    width = x.shape[1] // 2
    return x[:, :width] + x[:, width:]


def eye(width):
    rows = lax.broadcasted_iota(jnp.int32, (width, width), 0)
    cols = lax.broadcasted_iota(jnp.int32, (width, width), 1)
    return (rows == cols).astype(f32)


def total(x):
    return jnp.sum(jnp.sum(x, axis=0, keepdims=True), axis=1, keepdims=True)


class Table:
    def __init__(self, refs, phys, n):
        self.refs, self.phys, self.n = refs, phys, n

    def src(self, g, s, k):
        return self.refs[g][s * self.n + k]

    def dst(self, g, s, m):
        return self.refs[g][(self.phys + s) * self.n + m]


def gather_states(blocks, table, g, m, phys):
    return jnp.concatenate([blocks[s, table.dst(g, s, m)] for s in range(phys)], axis=1)


def scatter_states(store, product, table, g, m, phys, width):
    for s in range(phys):
        store[table.dst(g, s, m), s * width : (s + 1) * width, :] = product[
            :, s * width : (s + 1) * width
        ]


def chain_kernel(dims, first, last, *refs):
    hops, sizes, phys, n, own, width = dims
    count = hops * sizes
    table = Table(refs[:hops], phys, n)
    pos = refs[hops][0]
    refs = refs[hops + 1 :]
    local_left, local_right = refs[0], refs[1]
    moved = (None,) + refs[2 : 2 + count - 1]
    rest = refs[2 + count - 1 :]
    if not first:
        env_in, rest = rest[0], rest[1:]
    elif hops == 1:
        seeds, rest = rest[:2], rest[2:]
    out_ref, blocks, env, wide, tall = rest

    def slot(t):
        return pl.ds(lax.rem(pos - t + sizes, sizes) * own, own)

    def run(local, seed, step):
        for t in range(sizes):
            i = (hops - 1) * sizes + t
            if first:
                env[slot(t)] = seed[...] if i == 0 else moved[i][phys]
        if not first:
            env[...] = env_in[...]
        for g in reversed(range(hops)):
            for t in range(sizes):
                i = g * sizes + t
                blocks[g, :, slot(t)] = local[...] if i == 0 else moved[i][:phys]
            step(g)

    def left_step(g):
        for m in range(n):
            product = dot(env[m], gather_states(blocks.at[g], table, g, m, phys)).astype(bf16)
            scatter_states(tall, product, table, g, m, phys, width)
        for k in range(n):
            stacked = blocks[g, :, k].reshape(phys * width, width)
            env[k] = dot_tn(stacked, tall[k]).astype(bf16)

    def right_step(g):
        for k in range(n):
            stacked = blocks[g, :, k].reshape(phys * width, width)
            product = dot(stacked, env[k]).astype(bf16)
            for s in range(phys):
                wide[table.src(g, s, k), :, s * width : (s + 1) * width] = product[
                    s * width : (s + 1) * width
                ]
        for m in range(n):
            env[m] = dot_nt(wide[m], gather_states(blocks.at[g], table, g, m, phys)).astype(bf16)

    local_seeds = seeds if first and hops == 1 else (None, None)

    @pl.when(pos < sizes // 2)
    def _():
        run(local_left, local_seeds[0], left_step)

    @pl.when(pos >= sizes // 2)
    def _():
        run(local_right, local_seeds[1], right_step)

    if last:
        summed = env[0].astype(f32)
        for m in range(1, n):
            summed = summed + env[m].astype(f32)
        scale = (n * width) / total(summed * eye(width))
        for m in range(n):
            out_ref[m] = (env[m].astype(f32) * scale).astype(bf16)
    else:
        out_ref[...] = env[...]


def center_kernel(dims, tab_ref, pos_ref, onsite_ref, shift_ref, before_ref, *refs):
    sizes, phys, n, own, width = dims
    same_ref, cross_ref, mine_ref, swap_ref, bond_ref = refs[:5]
    site_parts = refs[5 : 5 + sizes]
    bond_parts = refs[5 + sizes : 5 + 2 * sizes]
    left_out, right_out = refs[5 + 2 * sizes : 7 + 2 * sizes]
    site, envs, bonds, tall, y_ref, z_ref, m_ref, scale_ref, factor_ref = refs[7 + 2 * sizes :]
    table = Table((tab_ref,), phys, n)
    pos = pos_ref[0]
    on_right = (pos >= sizes // 2).astype(jnp.int32)

    def slot(t, extra=0):
        return pl.ds(extra + lax.rem(pos - t + sizes, sizes) * own, own)

    envs[on_right] = same_ref[...]
    envs[1 - on_right] = cross_ref[...]
    envs[3 - on_right] = mine_ref[...]
    envs[2 + on_right] = swap_ref[...]
    bonds[0:own] = bond_ref[...]
    for t in range(sizes):
        site[:, slot(t)] = site_parts[t][...]
        bonds[slot(t, own)] = bond_parts[t][...]

    for repeat in range(NAPP):
        for m in range(n):
            product = dot(envs[0, m], gather_states(site, table, 0, m, phys)).astype(bf16)
            scatter_states(tall, product, table, 0, m, phys, width)
        for i in range(own):
            k = pos * own + i
            half = dot(envs[3, k], bonds[i]).astype(bf16)
            bonds[i] = (dot(half, envs[1, k]) + shift_ref[0] * bonds[i].astype(f32)).astype(bf16)
        for m in range(n):
            half = dot(envs[0, m], bonds[own + m]).astype(bf16)
            bonds[own + m] = (
                dot(half, envs[2, m]) + before_ref[0] * bonds[own + m].astype(f32)
            ).astype(bf16)
        for k in range(n):
            product = dot(tall[k], envs[1, k])
            for s in range(phys):
                site[s, k] = (
                    product[s * width : (s + 1) * width] + onsite_ref[s] * site[s, k].astype(f32)
                ).astype(bf16)

    count = 2 * (own + n)

    def gram(i):
        if i < own + n:
            return dot_nt(bonds[i], bonds[i])
        i -= own + n
        if i < own:
            stacked = site[:, pos * own + i].reshape(phys * width, width)
            return dot_tn(stacked, stacked)
        gathered = gather_states(site, table, 0, i - own, phys)
        return dot_nt(gathered, gathered)

    for i in range(count):
        g = gram(i)
        inverse = lax.rsqrt(total(g * g))
        scale_ref[i] = jnp.broadcast_to(jnp.sqrt(inverse), scale_ref.shape[1:])
        y = g * inverse
        y_ref[i] = split(y)
        z_ref[i] = split(1.5 * eye(width) - 0.5 * y)
    for i in range(count):
        y_ref[i] = split(fold(dot(z_ref[i], twice(y_ref[i]))))

    def middle():
        for i in range(count):
            m_ref[i] = split(1.5 * eye(width) - 0.5 * fold(dot(z_ref[i], twice(y_ref[i]))))

    def finish():
        for i in range(count):
            z_ref[i] = split(fold(dot(m_ref[i], twice(z_ref[i]))))

    def iterate(step, carry):
        middle()
        for i in range(count):
            y_ref[i] = split(fold(dot(m_ref[i], twice(y_ref[i]))))
        finish()
        return carry

    lax.fori_loop(0, NSI - 2, iterate, 0)
    middle()
    finish()

    for i in range(own + n):
        unit = dot(z_ref[i], twice(bonds[i])) * scale_ref[i][:1]
        y_ref[i] = split(unit)
    for i in range(own + n):
        grams = own + n + i
        parts = y_ref[i]
        if i < own:
            high, low = parts[:, :width], parts[:, width:]
            rows = jnp.concatenate(
                [
                    jnp.concatenate([high, high], axis=1),
                    jnp.concatenate([low, low], axis=1),
                ],
                axis=0,
            )
            factor = fold(dot_nt(z_ref[grams], rows)) * scale_ref[grams][:1]
        else:
            factor = jnp.transpose(fold(dot(z_ref[grams], twice(parts))) * scale_ref[grams][:1])
        factor_ref[i] = factor.astype(bf16)
    for i in range(own):
        k = pos * own + i
        stacked = site[:, k].reshape(phys * width, width)
        product = dot(stacked, factor_ref[i]).astype(bf16)
        for s in range(phys):
            left_out[s, i] = product[s * width : (s + 1) * width]
            right_out[s, i] = dot(factor_ref[own + table.src(0, s, k)], site[s, k]).astype(bf16)


def route(mesh_shape, target):
    sites, sizes = mesh_shape
    pairs = []
    for j in range(sites):
        for c in range(sizes):
            to = target(j, c)
            if to is not None:
                pairs.append((j * sizes + c, (to[0] % sites) * sizes + to[1] % sizes))
    return pairs


def per_device(
    mesh_shape,
    left_canon,
    right_canon,
    center_site,
    center_bond,
    left_seed,
    right_seed,
    left_sector,
    onsite,
    bond_shift,
):
    sites, sizes = mesh_shape
    half = sizes // 2
    steps = sites // 4
    hops = 2 if steps % 2 == 0 else 1
    left, right = left_canon[0], right_canon[0]
    phys, own, width = left.shape[0], left.shape[1], left.shape[2]
    src = left_sector[0]
    n = src.shape[1]
    labels = jnp.arange(n, dtype=jnp.int32)
    dst = jnp.sum(
        jnp.where(src[:, :, None] == labels[None, None, :], labels[None, :, None], 0), axis=1
    )
    tab = jnp.stack([src, dst]).reshape(-1)
    pos = lax.axis_index("sec").astype(jnp.int32)
    block = width * width * 2
    matrices = 2 * (own + n)
    chain_bytes = ((hops + 2) * phys * n + 3 * n) * block
    center_bytes = (2 * phys * n + 4 * n + 2 * (own + n) + 7 * matrices) * block
    spare = 6 * 2**20

    def params(held):
        return pltpu.CompilerParams(vmem_limit_bytes=held + spare)


    def move(x, target):
        return lax.ppermute(x, ("site", "sec"), route(mesh_shape, target))

    def outward(c, g):
        return g if c < half else -g

    moved, tables = [], [tab]
    for g in range(hops):
        for t in range(sizes):
            if g == 0 and t == 0:
                continue
            to_left = lax.rem(pos + t, sizes) < half
            payload = jnp.where(to_left, left, right)
            if g == hops - 1:
                seed = jnp.where(to_left, left_seed[0], right_seed[0])
                payload = jnp.concatenate([payload, seed[None]], axis=0)
            moved.append(
                move(payload, lambda j, c, g=g, t=t: (j + outward((c + t) % sizes, g), c + t))
            )
        if g > 0:
            tables.append(move(tab, lambda j, c, g=g: (j + outward(c, g), c)))
    shift_before = move(bond_shift, lambda j, c: (j + 1, c))

    dims = (hops, sizes, phys, n, own, width)
    env_shape = jax.ShapeDtypeStruct((n, width, width), bf16)
    count = hops * sizes
    env = None
    blocks_total = steps // hops
    for b in range(blocks_total):
        first, last = b == 0, b == blocks_total - 1
        extra, specs = (), []
        if not first:
            extra, specs = (env,), [VMEM]
        elif hops == 1:
            extra, specs = (left_seed[0], right_seed[0]), [VMEM, VMEM]
        env = pl.pallas_call(
            functools.partial(chain_kernel, dims, first, last),
            out_shape=env_shape,
            in_specs=[SMEM] * (hops + 1) + [VMEM] * (count + 1) + specs,
            out_specs=VMEM,
            scratch_shapes=[
                pltpu.VMEM((hops, phys, n, width, width), bf16),
                pltpu.VMEM((n, width, width), bf16),
                pltpu.VMEM((n, width, phys * width), bf16),
                pltpu.VMEM((n, phys * width, width), bf16),
            ],
            compiler_params=params(chain_bytes),
            name="chain_last" if last else "chain",
        )(*tables, pos[None], left, right, *moved, *extra)
        if first:
            center, bond, _ = lax.optimization_barrier((center_site[0], center_bond[0], env))
            center_parts = [center_site[0]] + [
                move(center, lambda j, c, t=t: (j, c + t)) for t in range(1, sizes)
            ]
            bond_parts = [
                move(center_bond[0] if t == 0 else bond, lambda j, c, t=t: (j + 1, c + t))
                for t in range(sizes)
            ]
        if not last:
            env = move(env, lambda j, c: (j + outward(c, hops), c))

    same = move(env, lambda j, c: (j + outward(c, 1), c))
    cross = move(env, lambda j, c: (j + outward(c, 1), c + half))
    swap = move(env, lambda j, c: (j, c + half))

    out_shape = jax.ShapeDtypeStruct((phys, own, width, width), bf16)
    left_new, right_new = pl.pallas_call(
        functools.partial(center_kernel, (sizes, phys, n, own, width)),
        out_shape=(out_shape, out_shape),
        in_specs=[SMEM] * 5 + [VMEM] * (5 + 2 * sizes),
        out_specs=(VMEM, VMEM),
        scratch_shapes=[
            pltpu.VMEM((phys, n, width, width), bf16),
            pltpu.VMEM((4, n, width, width), bf16),
            pltpu.VMEM((own + n, width, width), bf16),
            pltpu.VMEM((n, phys * width, width), bf16),
            pltpu.VMEM((matrices, width, 2 * width), bf16),
            pltpu.VMEM((matrices, width, 2 * width), bf16),
            pltpu.VMEM((matrices, width, 2 * width), bf16),
            pltpu.VMEM((matrices, 8, width), f32),
            pltpu.VMEM((own + n, width, width), bf16),
        ],
        compiler_params=params(center_bytes),
        name="center",
    )(
        tab,
        pos[None],
        onsite[0],
        bond_shift,
        shift_before,
        same,
        cross,
        env,
        swap,
        center_bond[0],
        *center_parts,
        *bond_parts,
    )
    return (left_new[None], right_new[None])


def solution(mesh):
    mesh_shape = (mesh.shape["site"], mesh.shape["sec"])
    return jax.shard_map(
        functools.partial(per_device, mesh_shape),
        mesh=mesh,
        in_specs=(
            P("site", None, "sec", None, None),
            P("site", None, "sec", None, None),
            P("site", None, "sec", None, None),
            P("site", "sec", None, None),
            P("site", "sec", None, None),
            P("site", "sec", None, None),
            P("site", None, None),
            P("site", None),
            P("site"),
        ),
        out_specs=(P("site", None, "sec", None, None), P("site", None, "sec", None, None)),
        check_vma=False,
    )
```

```python
import functools

import jax
import jax.numpy as jnp
from jax import lax
from jax.experimental import pallas as pl
from jax.experimental.pallas import tpu as pltpu
from jax.sharding import PartitionSpec as P

NSI = 10
NAPP = 2
f32 = jnp.float32
bf16 = jnp.bfloat16
VMEM = pl.BlockSpec(memory_space=pltpu.VMEM)
SMEM = pl.BlockSpec(memory_space=pltpu.SMEM)
HBM = pl.BlockSpec(memory_space=pltpu.HBM)


def dot(a, b):
    return jnp.dot(a, b, preferred_element_type=f32)


def dot_tn(a, b):
    return lax.dot_general(a, b, (((0,), (0,)), ((), ())), preferred_element_type=f32)


def dot_nt(a, b):
    return lax.dot_general(a, b, (((1,), (1,)), ((), ())), preferred_element_type=f32)


def split(x):
    high = x.astype(bf16)
    low = (x - high.astype(f32)).astype(bf16)
    return jnp.concatenate([high, low], axis=1)


def twice(s):
    return jnp.concatenate([s, s], axis=0)


def fold(x):
    width = x.shape[1] // 2
    return x[:, :width] + x[:, width:]


def eye(width):
    rows = lax.broadcasted_iota(jnp.int32, (width, width), 0)
    cols = lax.broadcasted_iota(jnp.int32, (width, width), 1)
    return (rows == cols).astype(f32)


def total(x):
    return jnp.sum(jnp.sum(x, axis=0, keepdims=True), axis=1, keepdims=True)


class Table:
    def __init__(self, refs, phys, n):
        self.refs, self.phys, self.n = refs, phys, n

    def src(self, g, s, k):
        return self.refs[g][s * self.n + k]

    def dst(self, g, s, m):
        return self.refs[g][(self.phys + s) * self.n + m]


def gather_states(blocks, table, g, m, phys):
    return jnp.concatenate([blocks[s, table.dst(g, s, m)] for s in range(phys)], axis=1)


def scatter_states(store, product, table, g, m, phys, width):
    for s in range(phys):
        store[table.dst(g, s, m), s * width : (s + 1) * width, :] = product[
            :, s * width : (s + 1) * width
        ]


def pack_kernel(routes, sizes, phys, pos_ref, *refs):
    sides, outs, sems = (refs[0:2], refs[2:4]), refs[4:-1], refs[-1]
    waits = []
    for i, (t, seeded) in enumerate(routes):
        to_left = lax.rem(pos_ref[0] + t, sizes) < sizes // 2
        for part in range(2 if seeded else 1):
            if not seeded:
                target = outs[i]
            else:
                target = outs[i].at[phys] if part else outs[i].at[pl.ds(0, phys)]
            sem = sems.at[2 * i + part]
            options = [pltpu.make_async_copy(ref, target, sem) for ref in sides[part]]
            pl.when(to_left)(options[0].start)
            pl.when(jnp.logical_not(to_left))(options[1].start)
            waits.append(options[0])
    for copy in waits:
        copy.wait()


def chain_kernel(dims, first, last, *refs):
    hops, sizes, phys, n, own, width = dims
    count = hops * sizes
    table = Table(refs[:hops], phys, n)
    pos = refs[hops][0]
    refs = refs[hops + 1 :]
    local_left, local_right = refs[0], refs[1]
    moved = (None,) + refs[2 : 2 + count - 1]
    rest = refs[2 + count - 1 :]
    if not first:
        env_in, rest = rest[0], rest[1:]
    elif hops == 1:
        seeds, rest = rest[:2], rest[2:]
    out_ref, blocks, env, wide, tall = rest

    def slot(t):
        return pl.ds(lax.rem(pos - t + sizes, sizes) * own, own)

    def run(local, seed, step):
        for t in range(sizes):
            i = (hops - 1) * sizes + t
            if first:
                env[slot(t)] = seed[...] if i == 0 else moved[i][phys]
        if not first:
            env[...] = env_in[...]
        for g in reversed(range(hops)):
            for t in range(sizes):
                i = g * sizes + t
                blocks[g, :, slot(t)] = local[...] if i == 0 else moved[i][:phys]
            step(g)

    def left_step(g):
        for m in range(n):
            product = dot(env[m], gather_states(blocks.at[g], table, g, m, phys)).astype(bf16)
            scatter_states(tall, product, table, g, m, phys, width)
        for k in range(n):
            stacked = blocks[g, :, k].reshape(phys * width, width)
            env[k] = dot_tn(stacked, tall[k]).astype(bf16)

    def right_step(g):
        for k in range(n):
            stacked = blocks[g, :, k].reshape(phys * width, width)
            product = dot(stacked, env[k]).astype(bf16)
            for s in range(phys):
                wide[table.src(g, s, k), :, s * width : (s + 1) * width] = product[
                    s * width : (s + 1) * width
                ]
        for m in range(n):
            env[m] = dot_nt(wide[m], gather_states(blocks.at[g], table, g, m, phys)).astype(bf16)

    local_seeds = seeds if first and hops == 1 else (None, None)

    @pl.when(pos < sizes // 2)
    def _():
        run(local_left, local_seeds[0], left_step)

    @pl.when(pos >= sizes // 2)
    def _():
        run(local_right, local_seeds[1], right_step)

    if last:
        summed = env[0].astype(f32)
        for m in range(1, n):
            summed = summed + env[m].astype(f32)
        scale = (n * width) / total(summed * eye(width))
        for m in range(n):
            out_ref[m] = (env[m].astype(f32) * scale).astype(bf16)
    else:
        out_ref[...] = env[...]


def center_kernel(dims, tab_ref, pos_ref, onsite_ref, shift_ref, before_ref, *refs):
    sizes, phys, n, own, width = dims
    same_ref, cross_ref, mine_ref, swap_ref, bond_ref = refs[:5]
    site_parts = refs[5 : 5 + sizes]
    bond_parts = refs[5 + sizes : 5 + 2 * sizes]
    left_out, right_out = refs[5 + 2 * sizes : 7 + 2 * sizes]
    site, envs, bonds, tall, y_ref, z_ref, m_ref, scale_ref, factor_ref = refs[7 + 2 * sizes :]
    table = Table((tab_ref,), phys, n)
    pos = pos_ref[0]
    on_right = (pos >= sizes // 2).astype(jnp.int32)

    def slot(t, extra=0):
        return pl.ds(extra + lax.rem(pos - t + sizes, sizes) * own, own)

    envs[on_right] = same_ref[...]
    envs[1 - on_right] = cross_ref[...]
    envs[3 - on_right] = mine_ref[...]
    envs[2 + on_right] = swap_ref[...]
    bonds[0:own] = bond_ref[...]
    for t in range(sizes):
        site[:, slot(t)] = site_parts[t][...]
        bonds[slot(t, own)] = bond_parts[t][...]

    for repeat in range(NAPP):
        for m in range(n):
            product = dot(envs[0, m], gather_states(site, table, 0, m, phys)).astype(bf16)
            scatter_states(tall, product, table, 0, m, phys, width)
        for i in range(own):
            k = pos * own + i
            half = dot(envs[3, k], bonds[i]).astype(bf16)
            bonds[i] = (dot(half, envs[1, k]) + shift_ref[0] * bonds[i].astype(f32)).astype(bf16)
        for m in range(n):
            half = dot(envs[0, m], bonds[own + m]).astype(bf16)
            bonds[own + m] = (
                dot(half, envs[2, m]) + before_ref[0] * bonds[own + m].astype(f32)
            ).astype(bf16)
        for k in range(n):
            product = dot(tall[k], envs[1, k])
            for s in range(phys):
                site[s, k] = (
                    product[s * width : (s + 1) * width] + onsite_ref[s] * site[s, k].astype(f32)
                ).astype(bf16)

    count = 2 * (own + n)

    def gram(i):
        if i < own + n:
            return dot_nt(bonds[i], bonds[i])
        i -= own + n
        if i < own:
            stacked = site[:, pos * own + i].reshape(phys * width, width)
            return dot_tn(stacked, stacked)
        gathered = gather_states(site, table, 0, i - own, phys)
        return dot_nt(gathered, gathered)

    for i in range(count):
        g = gram(i)
        inverse = lax.rsqrt(total(g * g))
        scale_ref[i] = jnp.broadcast_to(jnp.sqrt(inverse), scale_ref.shape[1:])
        y = g * inverse
        y_ref[i] = split(y)
        z_ref[i] = split(1.5 * eye(width) - 0.5 * y)
    for i in range(count):
        y_ref[i] = split(fold(dot(z_ref[i], twice(y_ref[i]))))

    def middle():
        for i in range(count):
            m_ref[i] = split(1.5 * eye(width) - 0.5 * fold(dot(z_ref[i], twice(y_ref[i]))))

    def finish():
        for i in range(count):
            z_ref[i] = split(fold(dot(m_ref[i], twice(z_ref[i]))))

    def iterate(step, carry):
        middle()
        for i in range(count):
            y_ref[i] = split(fold(dot(m_ref[i], twice(y_ref[i]))))
        finish()
        return carry

    lax.fori_loop(0, NSI - 2, iterate, 0)
    middle()
    finish()

    for i in range(own + n):
        unit = dot(z_ref[i], twice(bonds[i])) * scale_ref[i][:1]
        y_ref[i] = split(unit)
    for i in range(own + n):
        grams = own + n + i
        parts = y_ref[i]
        if i < own:
            high, low = parts[:, :width], parts[:, width:]
            rows = jnp.concatenate(
                [
                    jnp.concatenate([high, high], axis=1),
                    jnp.concatenate([low, low], axis=1),
                ],
                axis=0,
            )
            factor = fold(dot_nt(z_ref[grams], rows)) * scale_ref[grams][:1]
        else:
            factor = jnp.transpose(fold(dot(z_ref[grams], twice(parts))) * scale_ref[grams][:1])
        factor_ref[i] = factor.astype(bf16)
    for i in range(own):
        k = pos * own + i
        stacked = site[:, k].reshape(phys * width, width)
        product = dot(stacked, factor_ref[i]).astype(bf16)
        for s in range(phys):
            left_out[s, i] = product[s * width : (s + 1) * width]
            right_out[s, i] = dot(factor_ref[own + table.src(0, s, k)], site[s, k]).astype(bf16)


def route(mesh_shape, target):
    sites, sizes = mesh_shape
    pairs = []
    for j in range(sites):
        for c in range(sizes):
            to = target(j, c)
            if to is not None:
                pairs.append((j * sizes + c, (to[0] % sites) * sizes + to[1] % sizes))
    return pairs


def per_device(
    mesh_shape,
    left_canon,
    right_canon,
    center_site,
    center_bond,
    left_seed,
    right_seed,
    left_sector,
    onsite,
    bond_shift,
):
    sites, sizes = mesh_shape
    half = sizes // 2
    steps = sites // 4
    hops = 2 if steps % 2 == 0 else 1
    left, right = left_canon[0], right_canon[0]
    phys, own, width = left.shape[0], left.shape[1], left.shape[2]
    src = left_sector[0]
    n = src.shape[1]
    labels = jnp.arange(n, dtype=jnp.int32)
    dst = jnp.sum(
        jnp.where(src[:, :, None] == labels[None, None, :], labels[None, :, None], 0), axis=1
    )
    tab = jnp.stack([src, dst]).reshape(-1)
    pos = lax.axis_index("sec").astype(jnp.int32)
    block = width * width * 2
    matrices = 2 * (own + n)
    chain_bytes = ((hops + 2) * phys * n + 3 * n) * block
    center_bytes = (2 * phys * n + 4 * n + 2 * (own + n) + 7 * matrices) * block
    spare = 4 * 2**20

    def params(held):
        return pltpu.CompilerParams(vmem_limit_bytes=held + spare)


    def move(x, target):
        return lax.ppermute(x, ("site", "sec"), route(mesh_shape, target))

    def outward(c, g):
        return g if c < half else -g

    hops_sent = [(g, t) for g in range(hops) for t in range(sizes) if (g, t) != (0, 0)]
    routes = [(t, g == hops - 1) for g, t in hops_sent]
    payloads = pl.pallas_call(
        functools.partial(pack_kernel, routes, sizes, phys),
        out_shape=[
            jax.ShapeDtypeStruct((phys + int(seeded), own, width, width), bf16)
            for _, seeded in routes
        ],
        in_specs=[SMEM] + [HBM] * 4,
        out_specs=[VMEM] * len(routes),
        scratch_shapes=[pltpu.SemaphoreType.DMA((2 * len(routes),))],
        compiler_params=params(len(routes) * (phys + 1) * own * block),
        name="pack",
    )(
        pos[None],
        *[
            pltpu.with_memory_space_constraint(x, pltpu.HBM)
            for x in (left, right, left_seed[0], right_seed[0])
        ],
    )
    moved = [
        move(payload, lambda j, c, g=g, t=t: (j + outward((c + t) % sizes, g), c + t))
        for payload, (g, t) in zip(payloads, hops_sent)
    ]
    tables = [tab] + [
        move(tab, lambda j, c, g=g: (j + outward(c, g), c)) for g in range(1, hops)
    ]
    shift_before = move(bond_shift, lambda j, c: (j + 1, c))
    bond_same = move(center_bond[0], lambda j, c: (j + 1, c))
    moved, tables, shift_before, bond_same = lax.optimization_barrier(
        (moved, tables, shift_before, bond_same)
    )

    dims = (hops, sizes, phys, n, own, width)
    env_shape = jax.ShapeDtypeStruct((n, width, width), bf16)
    count = hops * sizes
    env = None
    blocks_total = steps // hops
    for b in range(blocks_total):
        first, last = b == 0, b == blocks_total - 1
        extra, specs = (), []
        if not first:
            extra, specs = (env,), [VMEM]
        elif hops == 1:
            extra, specs = (left_seed[0], right_seed[0]), [VMEM, VMEM]
        env = pl.pallas_call(
            functools.partial(chain_kernel, dims, first, last),
            out_shape=env_shape,
            in_specs=[SMEM] * (hops + 1) + [VMEM] * (count + 1) + specs,
            out_specs=VMEM,
            scratch_shapes=[
                pltpu.VMEM((hops, phys, n, width, width), bf16),
                pltpu.VMEM((n, width, width), bf16),
                pltpu.VMEM((n, width, phys * width), bf16),
                pltpu.VMEM((n, phys * width, width), bf16),
            ],
            compiler_params=params(chain_bytes),
            name="chain_last" if last else "chain",
        )(*tables, pos[None], left, right, *moved, *extra)
        if first:
            center, bond, _ = lax.optimization_barrier((center_site[0], center_bond[0], env))
            center_parts = [center_site[0]] + [
                move(center, lambda j, c, t=t: (j, c + t)) for t in range(1, sizes)
            ]
            bond_parts = [bond_same] + [
                move(bond, lambda j, c, t=t: (j + 1, c + t)) for t in range(1, sizes)
            ]
        if not last:
            env = move(env, lambda j, c: (j + outward(c, hops), c))
        if first:
            env, center_parts, bond_parts = lax.optimization_barrier(
                (env, center_parts, bond_parts)
            )

    same = move(env, lambda j, c: (j + outward(c, 1), c))
    cross = move(env, lambda j, c: (j + outward(c, 1), c + half))
    swap = move(env, lambda j, c: (j, c + half))

    out_shape = jax.ShapeDtypeStruct((phys, own, width, width), bf16)
    left_new, right_new = pl.pallas_call(
        functools.partial(center_kernel, (sizes, phys, n, own, width)),
        out_shape=(out_shape, out_shape),
        in_specs=[SMEM] * 5 + [VMEM] * (5 + 2 * sizes),
        out_specs=(VMEM, VMEM),
        scratch_shapes=[
            pltpu.VMEM((phys, n, width, width), bf16),
            pltpu.VMEM((4, n, width, width), bf16),
            pltpu.VMEM((own + n, width, width), bf16),
            pltpu.VMEM((n, phys * width, width), bf16),
            pltpu.VMEM((matrices, width, 2 * width), bf16),
            pltpu.VMEM((matrices, width, 2 * width), bf16),
            pltpu.VMEM((matrices, width, 2 * width), bf16),
            pltpu.VMEM((matrices, 8, width), f32),
            pltpu.VMEM((own + n, width, width), bf16),
        ],
        compiler_params=params(center_bytes),
        name="center",
    )(
        tab,
        pos[None],
        onsite[0],
        bond_shift,
        shift_before,
        same,
        cross,
        env,
        swap,
        center_bond[0],
        *center_parts,
        *bond_parts,
    )
    return (left_new[None], right_new[None])


def solution(mesh):
    mesh_shape = (mesh.shape["site"], mesh.shape["sec"])
    return jax.shard_map(
        functools.partial(per_device, mesh_shape),
        mesh=mesh,
        in_specs=(
            P("site", None, "sec", None, None),
            P("site", None, "sec", None, None),
            P("site", None, "sec", None, None),
            P("site", "sec", None, None),
            P("site", "sec", None, None),
            P("site", "sec", None, None),
            P("site", None, None),
            P("site", None),
            P("site"),
        ),
        out_specs=(P("site", None, "sec", None, None), P("site", None, "sec", None, None)),
        check_vma=False,
    )
```
